256 devices in a mesh: seq: 32 (over y, x, core), vocab: 8 (over z).
Axes of the slice: x: 4, y: 4, z: 8, core: 2. Of those that a mesh axis runs over, the one named last changes fastest.
Arguments:
- hidden: bfloat16 [4096, 8192], P('seq'), may hold values from -120 to 120
- head: bfloat16 [8192, 65536], P(None, ('seq', 'vocab')), may hold values from -0.5 to 0.5
- mask: int32 [4096], P('seq'), may hold values from 0 to 1, as said below
Outputs:
- positionwise_uncertainty: float32 [4096], P('seq')
- average_uncertainty_reward: float32 [], replicated
- derivative_wrt_latent_vectors: bfloat16 [4096, 8192], P('seq', 'vocab')
The draws below stay inside these ranges and needn't reach their ends.
Inputs may be any that keep to these rules, and one draw needn't show every extreme that they name: Among the 128 tokens of one index of seq at least half of 16 and at most 16 have mask 1, and the last index of seq has exactly 16; later indices have no fewer than earlier ones.
All inputs are finite; a program needn't handle non-finite values.
Results may differ from the reference program's by a relative error of at most 0.019.
Values may be sent and summed in bfloat16 or wider, within the bound.
A program may use at most 64 MiB of HBM per device.

```python
import jax
import jax.numpy as jnp
from jax import lax

D = 8192
TOK_DEV = 128
ACT_DEV = 16
TOKENS = 4096
VOCAB = 65536


def draw_hidden(key, part):
    first = jax.random.fold_in(key, 0)
    values = jnp.clip(jax.random.normal(first, (TOKENS, D), jnp.float32), -6.0, 6.0)
    return values.astype(jnp.bfloat16)


def draw_mask(key, part):
    block_list = TOKENS // TOK_DEV
    lowest = max(ACT_DEV // 2, 1)
    first, second = jax.random.split(jax.random.fold_in(key, 7))
    token_counts = jnp.sort(jax.random.randint(first, (block_list,), lowest, ACT_DEV + 1))
    token_counts = token_counts.at[block_list - 1].set(ACT_DEV)
    scores = jax.random.randint(second, (block_list, TOK_DEV), 0, 2 ** 20)
    scores = scores * TOK_DEV + jnp.arange(TOK_DEV, dtype=jnp.int32)[None, :]
    ranks = jnp.argsort(jnp.argsort(scores, axis=1), axis=1)
    response_indicator = (ranks < token_counts[:, None]).astype(jnp.int32)
    return response_indicator.reshape(TOKENS)


def shard_levels(own_key, shape, cuts, smallest, largest):
    gain, own = 1.0, jax.random.fold_in(own_key, 6)
    for axis_at, shards_of in cuts:
        draws = jnp.exp(jax.random.uniform(jax.random.fold_in(own, axis_at), (shards_of,), jnp.float32, smallest / len(cuts), largest / len(cuts)))
        gain = gain * jnp.repeat(draws, shape[axis_at] // shards_of).reshape([-1 if axis == axis_at else 1 for axis in range(len(shape))])
    return gain


def scatter_about(own_key, dims, spread, reach, cuts=(), kind=jnp.bfloat16):
    values = jax.random.normal(own_key, dims, jnp.float32) * spread
    if len(cuts) > 0:
        values = shard_levels(own_key, dims, cuts, -0.22, 0.18) * values
    return jnp.clip(values, min=-reach, max=reach).astype(kind)


def setup_inputs(seed: int = 0) -> dict:
    keys = jax.random.split(jax.random.key(seed), 4)
    return {
        "hidden": draw_hidden(jax.random.fold_in(keys[3], 71), 0),
        "head": scatter_about(keys[1], (D, VOCAB), (3.0 / D ** 0.5), 0.5, ((1, 256),)),
        "mask": draw_mask(jax.random.fold_in(keys[3], 71), 0),
    }


def reference(hidden, head, mask):
    logits = jnp.dot(hidden, head, preferred_element_type=jnp.float32)
    top = jnp.max(logits, axis=1)
    ex = jnp.exp(logits - top[:, None])
    total = jnp.sum(ex, axis=1)
    weighted = jnp.sum(ex * logits, axis=1)
    mean_logit = weighted / total
    distribution_uncertainty = top + jnp.log(total) - mean_logit
    inclusion_indicator = mask.astype(jnp.float32)
    positionwise_uncertainty = inclusion_indicator * distribution_uncertainty
    average_uncertainty_reward = jnp.sum(positionwise_uncertainty) / jnp.sum(inclusion_indicator)
    prob = ex / total[:, None]
    score_grad = (inclusion_indicator[:, None] * (-(prob * (logits - mean_logit[:, None])))).astype(jnp.bfloat16)
    derivative_wrt_latent_vectors = lax.dot_general(score_grad, head, (((1,), (1,)), ((), ())), preferred_element_type=jnp.float32)
    return positionwise_uncertainty, average_uncertainty_reward, derivative_wrt_latent_vectors.astype(jnp.bfloat16)
```

```python
import functools

import jax
import jax.numpy as jnp
from jax import lax
from jax.experimental import pallas as pl
from jax.experimental.pallas import tpu as pltpu
from jax.sharding import Mesh
from jax.sharding import PartitionSpec as P

MESH = pl.DeviceIdType.MESH
ACT = 16
Y, X, CORE, Z = "seq_0", "seq_1", "seq_2", "vocab"
SEQ = (Y, X, CORE)
SIDE = 4
F32 = jnp.float32
BF16 = jnp.bfloat16
N_SEMS = 192


def block_row(half, p, q):
    return ((q * SIDE + p) if half == 0 else (p * SIDE + q)) * ACT


def kernel(
    mask_ref, hidden_hbm, head_hbm, pos_ref, avg_ref, grad_ref,
    raw, gathered, head, logits, part, near_half, near_full, far_half, far_full, total_own, total_in, final,
    table, moved, stat_x, stat_y, stat_z, pair, local_sem, send_sem, recv_sem,
):
    y, x, core, z = (lax.axis_index(a) for a in (Y, X, CORE, Z))
    depth = 8
    tokens, width = raw.shape
    vocab_here = head.shape[2]
    cut = width // 2
    quarter = cut // 2
    slice_z = width // depth
    blocks = SIDE * SIDE
    rows_all = blocks * ACT

    def ring(axis, at, size, step):
        return {axis: lax.rem(at + (step + size), size)}

    other = {CORE: 1 - core}
    peers = [other]
    peers += [ring(X, x, SIDE, k) for k in (1, 2, 3)]
    peers += [ring(Y, y, SIDE, k) for k in (1, 2, 3)]
    peers += [ring(Z, z, depth, k) for k in range(1, depth)]

    load_hidden = pltpu.make_async_copy(hidden_hbm, raw, local_sem.at[0])
    load_hidden.start()
    load_head = pltpu.make_async_copy(head_hbm, head.at[0], local_sem.at[1])
    load_head.start()
    barrier = pltpu.get_barrier_semaphore()
    for peer in peers:
        pl.semaphore_signal(barrier, inc=1, device_id=peer, device_id_type=MESH)

    mask = mask_ref[...]
    mask_f = jnp.broadcast_to(mask.astype(F32), (8, tokens)).astype(BF16)
    before = lax.broadcasted_iota(jnp.int32, (tokens, tokens), 0)
    after = lax.broadcasted_iota(jnp.int32, (tokens, tokens), 1)
    upper = jnp.where(before <= after, 1.0, 0.0).astype(BF16)
    count = jnp.dot(mask_f, upper, preferred_element_type=F32)[0:1, :]
    slot = lax.broadcasted_iota(jnp.int32, (ACT, tokens), 0).astype(F32) + 1.0
    chosen = (jnp.broadcast_to(count, (ACT, tokens)) == slot) & (
        jnp.broadcast_to(mask, (ACT, tokens)) == 1
    )
    picker_f = jnp.where(chosen, 1.0, 0.0).astype(F32)
    picker = picker_f.astype(BF16)
    valid = jnp.sum(picker_f, axis=1, keepdims=True)

    load_hidden.wait()
    for c in range(0, width, 1024):
        gathered[0:ACT, c : c + 1024] = jnp.dot(
            picker, raw[:, c : c + 1024], preferred_element_type=F32
        ).astype(BF16)

    pl.semaphore_wait(barrier, len(peers))
    sent, number = [], [0]

    def send(source, target, device):
        k = number[0]
        number[0] += 1
        copy = pltpu.make_async_remote_copy(
            src_ref=source, dst_ref=target, send_sem=send_sem.at[k], recv_sem=recv_sem.at[k],
            device_id=device, device_id_type=MESH,
        )
        copy.start()
        sent.append(copy)
        return copy

    axes = ((X, x), (Y, y))

    def near(half, step):
        axis, at = axes[half]
        return ring(axis, at, SIDE, step)

    def far(half, step):
        axis, at = axes[1 - half]
        return ring(axis, at, SIDE, step)

    def piece(ref, half, p, q, low, high):
        r = block_row(half, p, q)
        return ref.at[r : r + ACT, half * cut + low : half * cut + high]

    got = {}

    def send_far(half, p):
        whole = piece(gathered, half, p, 0, 0, cut)
        got[half, p, 3] = send(whole, piece(gathered, half, p, 3, 0, cut), far(half, 1))
        got[half, p, 1] = send(whole, piece(gathered, half, p, 1, 0, cut), far(half, -1))

    for half in (0, 1):
        whole = piece(gathered, half, 0, 0, 0, cut)
        got[half, 3, 0] = send(whole, piece(gathered, half, 3, 0, 0, cut), near(half, 1))
        got[half, 1, 0] = send(whole, piece(gathered, half, 1, 0, 0, cut), near(half, -1))
    swap = send(head_hbm, head.at[1], other)
    for half in (0, 1):
        send_far(half, 0)
    for half in (0, 1):
        got[half, 3, 0].wait_recv()
        low = piece(gathered, half, 3, 0, 0, quarter), piece(gathered, half, 2, 0, 0, quarter)
        got[half, 2, 0, 0] = send(*low, near(half, 1))
        got[half, 1, 0].wait_recv()
        high = piece(gathered, half, 1, 0, quarter, cut), piece(gathered, half, 2, 0, quarter, cut)
        got[half, 2, 0, 1] = send(*high, near(half, -1))
    for p in (3, 1):
        for half in (0, 1):
            send_far(half, p)

    def forward(half, p):
        got[half, p, 3].wait_recv()
        low = piece(gathered, half, p, 3, 0, quarter), piece(gathered, half, p, 2, 0, quarter)
        got[half, p, 2, 0] = send(*low, far(half, 1))
        got[half, p, 1].wait_recv()
        high = piece(gathered, half, p, 1, quarter, cut), piece(gathered, half, p, 2, quarter, cut)
        got[half, p, 2, 1] = send(*high, far(half, -1))

    for half in (0, 1):
        forward(half, 0)
    for half in (0, 1):
        got[half, 2, 0, 0].wait_recv()
        got[half, 2, 0, 1].wait_recv()
        send_far(half, 2)
    for p in (3, 1, 2):
        for half in (0, 1):
            forward(half, p)
    for p in range(SIDE):
        for half in (0, 1):
            got[half, p, 2, 0].wait_recv()
            got[half, p, 2, 1].wait_recv()

    load_head.wait()
    swap.wait_recv()
    step_k = 1024
    for j in (0, 1):
        columns = slice(j * vocab_here, (j + 1) * vocab_here)
        logits[:, columns] = jnp.dot(
            gathered[:, 0:step_k], head[j, 0:step_k, :], preferred_element_type=F32
        )

        @pl.loop(1, width // step_k)
        def _(k):
            at = pl.ds(pl.multiple_of(k * step_k, step_k), step_k)
            logits[:, columns] += jnp.dot(
                gathered[:, at], head[j, at, :], preferred_element_type=F32
            )

    local = logits[...]
    top = jnp.max(local, axis=1, keepdims=True)
    ex = jnp.exp(local - top)
    sum_ex = jnp.sum(ex, axis=1, keepdims=True)
    sum_weighted = jnp.sum(ex * local, axis=1, keepdims=True)
    lane = lax.broadcasted_iota(jnp.int32, (rows_all, 128), 1)
    flags = jnp.concatenate([valid, jnp.zeros((rows_all - ACT, 1), F32)], axis=0)
    columns_in = jnp.where(
        lane == 0, top, jnp.where(lane == 1, sum_ex, jnp.where(lane == 2, sum_weighted, flags))
    )

    def absolute(r):
        dy, dx = divmod(r, SIDE)
        place = lax.rem(y + dy, SIDE) * SIDE + lax.rem(x + dx, SIDE)
        return pl.ds(pl.multiple_of(place * ACT, ACT), ACT)

    for r in range(blocks):
        table[absolute(r), :] = columns_in[r * ACT : (r + 1) * ACT, :]
    mine = table[...].T[0:8, :]

    def exchange(own, slots, axis, at, size):
        slots[at] = own
        for k in range(1, size):
            base = number[0]
            number[0] += 1
            pltpu.make_async_remote_copy(
                src_ref=slots.at[at], dst_ref=slots.at[at], send_sem=send_sem.at[base], recv_sem=recv_sem.at[base],
                device_id=ring(axis, at, size, k), device_id_type=MESH,
            ).start()
            came = lax.rem(at + (size - k), size)
            sent.append(
                pltpu.make_async_remote_copy(
                    src_ref=slots.at[at], dst_ref=slots.at[came], send_sem=send_sem.at[base], recv_sem=recv_sem.at[base],
                    device_id=ring(axis, at, size, k), device_id_type=MESH,
                )
            )
        for copy in sent[len(sent) - (size - 1) :]:
            copy.wait_recv()
        tops = [slots[k][0:1, :] for k in range(size)]
        best = functools.reduce(jnp.maximum, tops)
        scales = [jnp.exp(t - best) for t in tops]
        sums = sum(slots[k][1:2, :] * scales[k] for k in range(size))
        weights = sum(slots[k][2:3, :] * scales[k] for k in range(size))
        marks = functools.reduce(jnp.maximum, [slots[k][3:4, :] for k in range(size)])
        return jnp.concatenate([best, sums, weights, marks, jnp.zeros((4, best.shape[1]), F32)], axis=0)

    mine = exchange(mine, stat_x, X, x, SIDE)
    mine = exchange(mine, stat_y, Y, y, SIDE)
    mine = exchange(mine, stat_z, Z, z, depth)
    best, sums, weights, marks = (mine[k : k + 1, :] for k in range(4))
    mean = weights / sums
    entropy = best + jnp.log(sums) - mean
    summed = jnp.sum(entropy * marks, axis=1, keepdims=True)
    counted = jnp.sum(marks, axis=1, keepdims=True)
    row8 = lax.broadcasted_iota(jnp.int32, (8, 128), 0)
    pair[core] = jnp.where(row8 == 0, summed, counted)
    k_pair = number[0]
    number[0] += 1
    pltpu.make_async_remote_copy(
        src_ref=pair.at[core], dst_ref=pair.at[core], send_sem=send_sem.at[k_pair], recv_sem=recv_sem.at[k_pair],
        device_id=other, device_id_type=MESH,
    ).start()
    pair_in = pltpu.make_async_remote_copy(
        src_ref=pair.at[core], dst_ref=pair.at[1 - core], send_sem=send_sem.at[k_pair], recv_sem=recv_sem.at[k_pair],
        device_id=other, device_id_type=MESH,
    )
    sent.append(pair_in)

    back = jnp.concatenate([best, sums, mean, entropy, jnp.zeros((124, rows_all), F32)], axis=0)
    table[...] = back.T
    for r in range(blocks):
        moved[r * ACT : (r + 1) * ACT, :] = table[absolute(r), :]
    row_top, row_sum, row_mean = (moved[:, k : k + 1] for k in range(3))
    value = logits[...]
    score = (-((jnp.exp(value - row_top) / row_sum) * (value - row_mean))).astype(BF16)
    scores = [score[:, 0:vocab_here], score[:, vocab_here : 2 * vocab_here]]

    step_d = 512

    @pl.loop(0, width // step_d)
    def _(k):
        at = pl.ds(pl.multiple_of(k * step_d, step_d), step_d)
        both = [
            lax.dot_general(scores[j], head[j, at, :], (((1,), (1,)), ((), ())), preferred_element_type=F32)
            for j in (0, 1)
        ]
        part[:, at] = (both[0] + both[1]).astype(BF16)

    def add_into(target, source):
        target[...] = (target[...].astype(F32) + source[...].astype(F32)).astype(BF16)

    order = (2, 1, 3, 0)
    half_in, full_in, near_in = {}, {}, {}
    for p in order:
        for half in (0, 1):
            half_in[half, p, 1] = send(
                piece(part, half, p, 2, 0, quarter), far_half.at[half, p, 0], far(half, 1)
            )
            half_in[half, p, 3] = send(
                piece(part, half, p, 2, quarter, cut), far_half.at[half, p, 1], far(half, -1)
            )
    for p in order:
        for half in (0, 1):
            half_in[half, p, 1].wait_recv()
            add_into(piece(part, half, p, 1, 0, quarter), far_half.at[half, p, 0])
            full_in[half, p, 0] = send(piece(part, half, p, 1, 0, cut), far_full.at[half, p, 0], far(half, 1))
            half_in[half, p, 3].wait_recv()
            add_into(piece(part, half, p, 3, quarter, cut), far_half.at[half, p, 1])
            full_in[half, p, 1] = send(piece(part, half, p, 3, 0, cut), far_full.at[half, p, 1], far(half, -1))
    for p in order:
        for half in (0, 1):
            for side in (0, 1):
                full_in[half, p, side].wait_recv()
            mine_ref = piece(part, half, p, 0, 0, cut)
            ends = far_full[half, p, 0].astype(F32) + far_full[half, p, 1].astype(F32)
            mine_ref[...] = (mine_ref[...].astype(F32) + ends).astype(BF16)
            if p == 2:
                near_in[half, 1] = send(piece(part, half, 2, 0, 0, quarter), near_half.at[half, 0], near(half, 1))
                near_in[half, 3] = send(piece(part, half, 2, 0, quarter, cut), near_half.at[half, 1], near(half, -1))
            if p == 1:
                near_in[half, 1].wait_recv()
                add_into(piece(part, half, 1, 0, 0, quarter), near_half.at[half, 0])
                near_in[half, 0, 0] = send(piece(part, half, 1, 0, 0, cut), near_full.at[half, 0], near(half, 1))
            if p == 3:
                near_in[half, 3].wait_recv()
                add_into(piece(part, half, 3, 0, quarter, cut), near_half.at[half, 1])
                near_in[half, 0, 1] = send(piece(part, half, 3, 0, 0, cut), near_full.at[half, 1], near(half, -1))
    for half in (0, 1):
        near_in[half, 0, 0].wait_recv()
        near_in[half, 0, 1].wait_recv()
        ends = near_full[half, 0].astype(F32) + near_full[half, 1].astype(F32)
        own = (piece(part, half, 0, 0, 0, cut)[...].astype(F32) + ends).astype(BF16)
        for k in range(depth // 2):
            total_own[half * (depth // 2) + k] = own[:, k * slice_z : (k + 1) * slice_z]

    arrivals = []
    for k in range(1, depth):
        s = number[0]
        number[0] += 1
        target = lax.rem(z + k, depth)
        copy = pltpu.make_async_remote_copy(
            src_ref=total_own.at[target], dst_ref=total_in.at[k - 1], send_sem=send_sem.at[s], recv_sem=recv_sem.at[s],
            device_id={Z: target}, device_id_type=MESH,
        )
        copy.start()
        sent.append(copy)
        arrivals.append(copy)

    pair_in.wait_recv()
    sums_of = pair[0] + pair[1]
    avg_ref[...] = sums_of[0:1, :] / sums_of[1:2, :]
    pos_ref[...] = jnp.sum(picker_f * moved[0:ACT, 3:4], axis=0, keepdims=True)
    spread = picker_f.T.astype(BF16)

    gradient = total_own[z].astype(F32)
    for k, copy in enumerate(arrivals):
        copy.wait_recv()
        gradient = gradient + total_in[k].astype(F32)
    grad_ref[...] = jnp.dot(spread, gradient.astype(BF16), preferred_element_type=F32).astype(BF16)
    for copy in sent:
        copy.wait_send()


def body(hidden, head, mask):
    tokens, width = hidden.shape
    vocab_here = head.shape[1]
    depth = lax.axis_size(Z)
    blocks = SIDE * SIDE
    cut = width // 2
    quarter = cut // 2
    vmem = functools.partial(pl.BlockSpec, memory_space=pltpu.VMEM)
    hbm = functools.partial(pl.BlockSpec, memory_space=pl.ANY)
    pos, avg, grad = pl.pallas_call(
        kernel,
        out_shape=(
            jax.ShapeDtypeStruct((1, tokens), F32),
            jax.ShapeDtypeStruct((1, 128), F32),
            jax.ShapeDtypeStruct((tokens, width // depth), BF16),
        ),
        in_specs=[vmem(), hbm(), hbm()],
        out_specs=(vmem(), vmem(), vmem()),
        scratch_shapes=[
            pltpu.VMEM((tokens, width), BF16),
            pltpu.VMEM((blocks * ACT, width), BF16),
            pltpu.VMEM((2, width, vocab_here), BF16),
            pltpu.VMEM((blocks * ACT, 2 * vocab_here), F32),
            pltpu.VMEM((blocks * ACT, width), BF16),
            pltpu.VMEM((2, 2, ACT, quarter), BF16),
            pltpu.VMEM((2, 2, ACT, cut), BF16),
            pltpu.VMEM((2, SIDE, 2, ACT, quarter), BF16),
            pltpu.VMEM((2, SIDE, 2, ACT, cut), BF16),
            pltpu.VMEM((depth, ACT, width // depth), BF16),
            pltpu.VMEM((depth - 1, ACT, width // depth), BF16),
            pltpu.VMEM((ACT, width // depth), F32),
            pltpu.VMEM((blocks * ACT, 128), F32),
            pltpu.VMEM((blocks * ACT, 128), F32),
            pltpu.VMEM((SIDE, 8, blocks * ACT), F32),
            pltpu.VMEM((SIDE, 8, blocks * ACT), F32),
            pltpu.VMEM((depth, 8, blocks * ACT), F32),
            pltpu.VMEM((2, 8, 128), F32),
            pltpu.SemaphoreType.DMA((2,)),
            pltpu.SemaphoreType.DMA((N_SEMS,)),
            pltpu.SemaphoreType.DMA((N_SEMS,)),
        ],
        compiler_params=pltpu.CompilerParams(
            collective_id=0, has_side_effects=True, vmem_limit_bytes=60 * 2**20
        ),
        name="entropy_bonus",
    )(mask.reshape(1, tokens), hidden, head)
    return pos.reshape(tokens), avg[0, 0], grad


def solution(mesh):
    finer = Mesh(mesh.devices.reshape(SIDE, SIDE, 2, mesh.shape["vocab"]), (Y, X, CORE, Z))
    return jax.shard_map(
        body,
        mesh=finer,
        in_specs=(P(SEQ, None), P(None, (*SEQ, Z)), P(SEQ)),
        out_specs=(P(SEQ), P(), P(SEQ, Z)),
        check_vma=False,
    )
```
